32 devices in a mesh: ea: 8 (over z, y), sa: 4 (over x, core).
Axes of the slice: x: 2, y: 2, z: 4, core: 2. Of those that a mesh axis runs over, the one named last changes fastest.
Arguments:
- lesser: bfloat16 [2, 1024, 2, 256, 256], P(None, 'ea', None, 'sa'), may hold values from -30 to 30, as said below
- greater: bfloat16 [2, 1024, 2, 256, 256], P(None, 'ea', None, 'sa'), may hold values from -30 to 30, as said below
Outputs:
- polar: float32 [2, 1024, 2, 256, 256], P(None, 'ea', None, 'sa')
- pol_norm: float32 [1], replicated
The draws below stay inside these ranges and needn't reach their ends.
Inputs may be any that keep to these rules, and one draw needn't show every extreme that they name: `lesser`: Real-valued entries, independent from energy to energy. `greater`: Real-valued entries, independent from energy to energy.
All inputs are finite; a program needn't handle non-finite values.
Results may differ from the reference program's by a relative error of at most 0.0049.
Values may be sent and summed in bfloat16 or wider, within the bound.
A program may use at most 320 MiB of HBM per device.

```python
import math
import jax
import jax.numpy as jnp
from jax import lax

NE = 1024
ORB = 256
BLOCKS = 2


def green_draw(key):
    first, second = jax.random.split(key, 2)
    shape = (2, NE, BLOCKS, ORB, ORB)
    rows = jnp.arange(ORB, dtype=jnp.float32) / ORB
    row_scale = 10.0 ** (0.5 * rows - 0.25)
    values = jax.random.truncated_normal(first, -4.0, 4.0, shape, jnp.float32)
    column_scale = 10.0 ** (jax.random.uniform(second, (1, 1, BLOCKS, 1, ORB), jnp.float32) - 0.5)
    return values * row_scale[None, None, None, :, None] * column_scale


def draw_lesser(key, part):
    return green_draw(jax.random.fold_in(key, 11)).astype(jnp.bfloat16)


def draw_greater(key, part):
    return green_draw(jax.random.fold_in(key, 23)).astype(jnp.bfloat16)


def setup_inputs(seed: int = 0) -> dict:
    keys = jax.random.split(jax.random.key(seed), 3)
    return {
        "lesser": draw_lesser(jax.random.fold_in(keys[2], 71), 0),
        "greater": draw_greater(jax.random.fold_in(keys[2], 71), 0),
    }


def energy_tables(count):
    index = jnp.arange(count, dtype=jnp.int32)
    phase = index[:, None] * index[None, :] % count
    angle = phase.astype(jnp.float32) * (2.0 * math.pi / count)
    return (jnp.cos(angle).astype(jnp.bfloat16), jnp.sin(angle).astype(jnp.bfloat16))

def spectra(columns, cosine, sine):
    stacked = jnp.concatenate(columns, axis=1)
    return (jnp.dot(cosine, stacked, preferred_element_type=jnp.float32), jnp.dot(sine, stacked, preferred_element_type=jnp.float32))

def split_spectrum(cos_part, sin_part, which, width):
    real_cols = slice(2 * which * width, (2 * which + 1) * width)
    imag_cols = slice((2 * which + 1) * width, (2 * which + 2) * width)
    spec_re = cos_part[:, real_cols] + sin_part[:, imag_cols]
    spec_im = cos_part[:, imag_cols] - sin_part[:, real_cols]
    return (spec_re, spec_im)

def polarize(less_re, less_im, great_re, great_im, cosine, sine, count):
    width = less_re.shape[1]
    prod_re = (less_re * great_re + less_im * great_im).astype(jnp.bfloat16)
    prod_im = (less_im * great_re - less_re * great_im).astype(jnp.bfloat16)
    cos_part, sin_part = spectra([prod_re, prod_im], cosine, sine)
    corr_re = cos_part[:, :width] - sin_part[:, width:]
    corr_im = cos_part[:, width:] + sin_part[:, :width]
    weight = float(count) ** (-1.5)
    return jnp.stack([weight * corr_im, -weight * corr_re])

def reference(lesser, greater):
    cosine, sine = energy_tables(NE)
    group = ORB * 16
    groups = BLOCKS * ORB * ORB // group
    less_groups = lesser.reshape(2, NE, groups, group).transpose(2, 0, 1, 3)
    great_groups = greater.reshape(2, NE, groups, group).transpose(2, 0, 1, 3)

    def one_group(pair):
        less_part, great_part = pair
        cos_part, sin_part = spectra([less_part[0], less_part[1], great_part[0], great_part[1]], cosine, sine)
        less_re, less_im = split_spectrum(cos_part, sin_part, 0, group)
        great_re, great_im = split_spectrum(cos_part, sin_part, 1, group)
        return polarize(less_re, less_im, great_re, great_im, cosine, sine, NE)
    polar_groups = lax.map(one_group, (less_groups, great_groups))
    polar = polar_groups.transpose(1, 2, 0, 3).reshape(2, NE, BLOCKS, ORB, ORB)
    total = jnp.sum(polar * polar)
    pol_norm = jnp.sqrt(total / (NE * BLOCKS * ORB * ORB) + 1e-06).reshape(1)
    return (polar, pol_norm)
```

```python
import functools
import math

import jax
import jax.numpy as jnp
from jax import lax
from jax.experimental import pallas as pl
from jax.experimental.pallas import tpu as pltpu
from jax.sharding import PartitionSpec as P

LANES = 128


def energy_tables(count):
    index = jnp.arange(count, dtype=jnp.int32)
    phase = index[:, None] * index[None, :] % count
    angle = phase.astype(jnp.float32) * (2.0 * math.pi / count)
    return (jnp.cos(angle).astype(jnp.bfloat16), jnp.sin(angle).astype(jnp.bfloat16))


def pack_kernel(peers, per, less_ref, great_ref, *rest):
    target, wide = rest[-2:]
    for index, source in enumerate((less_ref, great_ref)):
        for part in range(2):
            wide[...] = source[part, :, 0].astype(jnp.float32)
            field = 2 * index + part
            for peer in range(peers):
                for row in range(per):
                    at = (4 * row + field) * LANES
                    target[peer, :, at : at + LANES] = wide[
                        :, peer * per + row, :
                    ].astype(jnp.bfloat16)


def pack(lesser, greater, block, half, peers, after):
    _, energies, _, rows, _ = lesser.shape
    per = rows // peers
    width = per * 4 * LANES
    step = min(32, energies)
    source = pl.BlockSpec((2, step, 1, rows, LANES), lambda e: (0, e, block, 0, half))
    out = jax.ShapeDtypeStruct((peers, energies, width), jnp.bfloat16)
    return pl.pallas_call(
        functools.partial(pack_kernel, peers, per),
        grid=(energies // step,),
        out_shape=out,
        in_specs=[source, source]
        + [pl.BlockSpec(memory_space=pl.ANY) for _ in after],
        out_specs=pl.BlockSpec((peers, step, width), lambda e: (0, e, 0)),
        scratch_shapes=[pltpu.VMEM((step, rows, LANES), jnp.float32)],
        cost_estimate=pl.CostEstimate(
            flops=0, bytes_accessed=4 * out.size, transcendentals=0
        ),
        name="pack",
    )(lesser, greater, *after)


def unpack_kernel(peers, per, source, *rest):
    target = rest[-1]
    for part in range(2):
        for peer in range(peers):
            for row in range(per):
                at = (2 * row + part) * LANES
                target[part, :, 0, peer * per + row, :] = source[
                    peer, :, at : at + LANES
                ].astype(jnp.float32)


def unpack(arrived, polar, block, half, shape):
    peers, energies, width = arrived.shape
    rows = shape[3]
    per = rows // peers
    step = min(32, energies)
    extra = [] if polar is None else [polar]
    return pl.pallas_call(
        functools.partial(unpack_kernel, peers, per),
        grid=(energies // step,),
        out_shape=jax.ShapeDtypeStruct(shape, jnp.float32),
        in_specs=[pl.BlockSpec((peers, step, width), lambda e: (0, e, 0))]
        + [pl.BlockSpec(memory_space=pl.ANY) for _ in extra],
        out_specs=pl.BlockSpec(
            (2, step, 1, rows, LANES), lambda e: (0, e, block, 0, half)
        ),
        input_output_aliases={1: 0} if extra else {},
        cost_estimate=pl.CostEstimate(
            flops=0, bytes_accessed=6 * arrived.size, transcendentals=0
        ),
        name="unpack",
    )(arrived, *extra)


def correlate_kernel(tile, weight, cosine, sine, columns, sent, total, prod):
    w = LANES
    count = cosine.shape[0]

    @pl.when(pl.program_id(0) == 0)
    def _():
        total[...] = jnp.zeros_like(total)

    @pl.loop(0, count // tile)
    def _(k):
        rows = pl.ds(pl.multiple_of(k * tile, tile), tile)
        c = jnp.dot(cosine[rows, :], columns[...], preferred_element_type=jnp.float32)
        s = jnp.dot(sine[rows, :], columns[...], preferred_element_type=jnp.float32)
        less_re = c[:, :w] + s[:, w : 2 * w]
        less_im = c[:, w : 2 * w] - s[:, :w]
        great_re = c[:, 2 * w : 3 * w] + s[:, 3 * w :]
        great_im = c[:, 3 * w :] - s[:, 2 * w : 3 * w]
        prod[rows, :w] = (less_re * great_re + less_im * great_im).astype(jnp.bfloat16)
        prod[rows, w:] = (less_im * great_re - less_re * great_im).astype(jnp.bfloat16)

    @pl.loop(0, count // tile)
    def _(k):
        rows = pl.ds(pl.multiple_of(k * tile, tile), tile)
        c = jnp.dot(cosine[rows, :], prod[...], preferred_element_type=jnp.float32)
        s = jnp.dot(sine[rows, :], prod[...], preferred_element_type=jnp.float32)
        polar_re = weight * (c[:, w:] + s[:, :w])
        polar_im = -weight * (c[:, :w] - s[:, w:])
        square = polar_re * polar_re + polar_im * polar_im
        total[...] += jnp.sum(square.reshape(tile // 8, 8, w), axis=0)
        sent[rows, :w] = polar_re.astype(jnp.bfloat16)
        sent[rows, w:] = polar_im.astype(jnp.bfloat16)


def correlate(columns, cosine, sine):
    count, width = columns.shape
    steps = width // (4 * LANES)
    table = pl.BlockSpec((count, count), lambda t: (0, 0))
    return pl.pallas_call(
        functools.partial(correlate_kernel, min(512, count), float(count) ** (-1.5)),
        grid=(steps,),
        out_shape=(
            jax.ShapeDtypeStruct((count, width // 2), jnp.bfloat16),
            jax.ShapeDtypeStruct((8, LANES), jnp.float32),
        ),
        in_specs=[table, table, pl.BlockSpec((count, 4 * LANES), lambda t: (0, t))],
        out_specs=(
            pl.BlockSpec((count, 2 * LANES), lambda t: (0, t)),
            pl.BlockSpec((8, LANES), lambda t: (0, 0)),
        ),
        scratch_shapes=[pltpu.VMEM((count, 2 * LANES), jnp.bfloat16)],
        compiler_params=pltpu.CompilerParams(vmem_limit_bytes=50 * 1024 * 1024),
        cost_estimate=pl.CostEstimate(
            flops=6 * count * count * width,
            bytes_accessed=3 * count * width,
            transcendentals=0,
        ),
        name="correlate",
    )(cosine, sine, columns)


def exchange(values):
    return lax.all_to_all(values, "ea", split_axis=0, concat_axis=0, tiled=True)


def solution(mesh):
    peers = mesh.shape["ea"]
    everyone = peers * mesh.shape["sa"]

    def body(lesser, greater):
        shape = lesser.shape
        count = shape[1] * peers
        entries = lesser.size // 2 * everyone
        chunks = [
            (block, half) for block in range(shape[2]) for half in range(shape[4] // LANES)
        ]
        totals = []
        returned = []
        arrived = []

        def send(index):
            after = [totals[index - 2]] if index >= 2 else []
            values = pack(lesser, greater, *chunks[index], peers, after)
            arrived.append(exchange(values))

        send(0)
        cosine, sine = lax.optimization_barrier(energy_tables(count))
        for index in range(len(chunks)):
            if index + 1 < len(chunks):
                send(index + 1)
            columns = arrived[index]
            sent, total = correlate(columns.reshape(count, -1), cosine, sine)
            totals.append(total)
            returned.append(exchange(sent.reshape(peers, shape[1], -1)))
        polar = None
        for (block, half), piece in zip(chunks, returned):
            polar = unpack(piece, polar, block, half, shape)
        total = jnp.sum(sum(totals))
        parts = lax.all_to_all(
            jnp.broadcast_to(total, (everyone, LANES)),
            ("ea", "sa"),
            split_axis=0,
            concat_axis=0,
            tiled=True,
        )
        norm_total = jnp.sum(parts[:, 0])
        pol_norm = jnp.sqrt(norm_total / entries + 1e-06).reshape(1)
        return (polar, pol_norm)

    return jax.shard_map(
        body,
        mesh=mesh,
        in_specs=(P(None, "ea", None, "sa", None), P(None, "ea", None, "sa", None)),
        out_specs=(P(None, "ea", None, "sa", None), P()),
        check_vma=False,
    )
```
